32 devices in a mesh: seg: 4 (over y, core), vid: 4 (over z), tp: 2 (over x).
Axes of the slice: x: 2, y: 2, z: 4, core: 2. Of those that a mesh axis runs over, the one named last changes fastest.
Arguments:
- tokens: bfloat16 [4, 2048, 2048], P('vid', 'seg', 'tp'), may hold values from -400 to 400
- key_weight: bfloat16 [2048, 2048], P('vid', 'tp'), may hold values from -0.125 to 0.125
- query_weight: bfloat16 [2048, 2048], P('vid', 'tp'), may hold values from -0.125 to 0.125
- latent_queries: bfloat16 [128, 2048], P(None, 'tp'), may hold values from -400 to 400
- init_memory: float32 [4, 128, 2048], P('vid', None, 'tp'), may hold values from -6 to 6
- forget: float32 [4, 4, 2048], P('vid', 'seg', 'tp'), may hold values from 0 to 1
Outputs:
- mixed: bfloat16 [4, 2048, 2048], P('vid', 'seg', 'tp')
- memory: float32 [4, 512, 2048], P('vid', 'seg', 'tp')
The draws below stay inside these ranges and needn't reach their ends.
All inputs are finite; a program needn't handle non-finite values.
Results may differ from the reference program's by a relative error of at most 0.015.
The reference program's roundings to bfloat16 on the way count: a program that leaves them out, or rounds other values in their place, can miss the bound.
Values may be sent and summed in bfloat16 or wider, within the bound.
A program may use at most 64 MiB of HBM per device.

```python
import jax
import jax.numpy as jnp
from jax import lax

D = 2048
HEAD = 128
M = 128
TOK = 512
HEADS = 16
SEGMENT_COUNT = 4
VIDEO_COUNT = 4
FRAMES = 2048


def draw_tokens(key, part):
    base = jax.random.normal(jax.random.fold_in(key, 11), (VIDEO_COUNT, FRAMES, D), jnp.float32)
    return jnp.clip(base, -400.0, 400.0).astype(jnp.bfloat16)


def draw_latent_queries(key, part):
    base = jax.random.normal(jax.random.fold_in(key, 21), (M, D), jnp.float32)
    return jnp.clip(base, -400.0, 400.0).astype(jnp.bfloat16)


def draw_forget(key, part):
    slow = 0.1 ** (1.0 / SEGMENT_COUNT)
    low = 0.02
    level = jax.random.uniform(jax.random.fold_in(key, 31), (VIDEO_COUNT, 1, D), jnp.float32)
    rate = jnp.exp(jnp.log(low) + level * (jnp.log(slow) - jnp.log(low)))
    power = jax.random.uniform(jax.random.fold_in(key, 32), (VIDEO_COUNT, SEGMENT_COUNT, D), jnp.float32, 0.5, 1.0)
    retained_memory = rate ** power
    segment_group = jax.random.randint(jax.random.fold_in(key, 33), (VIDEO_COUNT, SEGMENT_COUNT, 1), 0, 6) == 0
    training_loss = jax.random.uniform(jax.random.fold_in(key, 34), (VIDEO_COUNT, SEGMENT_COUNT, 1), jnp.float32, 0.5, 0.8)
    return retained_memory * jnp.where(segment_group, training_loss, 1.0)


def steps_of(stream_key, shape, pieces, smallest, largest):
    gain = 1.0
    for axis_at, parts in pieces:
        heights = jax.random.uniform(jax.random.fold_in(jax.random.fold_in(stream_key, 6), axis_at), (parts,), jnp.float32, smallest / len(pieces), largest / len(pieces))
        gain = gain * jnp.repeat(jnp.exp(heights), shape[axis_at] // parts).reshape((-1,) + (1,) * (len(shape) - 1 - axis_at))
    return gain


def bell_draw(key, shape, deviation, bound, split=(), held_as=jnp.bfloat16):
    result = deviation * jax.random.normal(key, shape, jnp.float32)
    if split:
        result = result * steps_of(key, shape, split, -0.22, 0.18)
    return jnp.clip(result, -bound, bound).astype(held_as)


def setup_inputs(seed: int = 0) -> dict:
    splits = jax.random.split(jax.random.key(seed), 7)
    tokens = draw_tokens(jax.random.fold_in(splits[6], 71), 0)
    key_weight = bell_draw(splits[1], (D, D), D ** -0.5, 0.125, ((0, 4), (1, 2)))
    query_weight = bell_draw(splits[2], (D, D), D ** -0.5, 0.125, ((0, 4), (1, 2)))
    latent_queries = draw_latent_queries(jax.random.fold_in(splits[6], 71), 0)
    init_memory = bell_draw(splits[4], (VIDEO_COUNT, M, D), 1.0, 6.0, ((0, 4), (2, 2)), jnp.float32)
    forget = draw_forget(jax.random.fold_in(splits[6], 71), 0)
    return dict(tokens=tokens, key_weight=key_weight, query_weight=query_weight, latent_queries=latent_queries, init_memory=init_memory, forget=forget)


def rounded(value):
    return lax.optimization_barrier(value.astype(jnp.bfloat16)).astype(jnp.float32)

def trailing_softmax(scores):
    top = lax.optimization_barrier(jnp.max(scores, axis=-1, keepdims=True))
    expo = jnp.exp(scores - top)
    return expo / lax.optimization_barrier(jnp.sum(expo, axis=-1, keepdims=True))

def resample(latent, keys, values):
    scores = jnp.einsum('mhe,the->hmt', latent, keys) / jnp.sqrt(jnp.float32(HEAD))
    weight_params = rounded(trailing_softmax(scores))
    return jnp.einsum('hmt,the->mhe', weight_params, values)

def readout(queries, memory_in):
    heads = memory_in.reshape(M, HEADS, HEAD)
    normed = heads * lax.rsqrt(lax.optimization_barrier(jnp.mean(heads * heads, axis=-1, keepdims=True)) + 1e-06)
    scores = jnp.einsum('the,mhe->htm', queries, rounded(normed)) / jnp.sqrt(jnp.float32(HEAD))
    weight_params = rounded(trailing_softmax(scores))
    return jnp.einsum('htm,mhe->the', weight_params, rounded(heads))

def reference(tokens, key_weight, query_weight, latent_queries, init_memory, forget):
    latent = latent_queries.astype(jnp.float32).reshape(M, HEADS, HEAD)

    def video(items):
        frames, initial_memory, retain = items
        keys = jnp.dot(frames, key_weight, preferred_element_type=jnp.float32).astype(jnp.bfloat16).astype(jnp.float32)
        queries = jnp.dot(frames, query_weight, preferred_element_type=jnp.float32).astype(jnp.bfloat16).astype(jnp.float32)
        keys = keys.reshape(SEGMENT_COUNT, TOK, HEADS, HEAD)
        queries = queries.reshape(SEGMENT_COUNT, TOK, HEADS, HEAD)
        values = frames.astype(jnp.float32).reshape(SEGMENT_COUNT, TOK, HEADS, HEAD)

        def step(memory_in, segment):
            seg_keys, seg_queries, seg_values, seg_retain = segment
            update = resample(latent, seg_keys, seg_values).reshape(M, D)
            read = readout(seg_queries, memory_in).reshape(TOK, D)
            mixed = (seg_values.reshape(TOK, D) + read).astype(jnp.bfloat16)
            memory_out = seg_retain[None, :] * memory_in + update
            return (memory_out, (mixed, memory_out))
        last, (mixed, memory) = lax.scan(step, initial_memory, (keys, queries, values, retain))
        return (mixed.reshape(FRAMES, D), memory.reshape(SEGMENT_COUNT * M, D))
    return lax.map(video, (tokens, init_memory, forget))
```

```python
import functools

import jax
import jax.numpy as jnp
from jax import lax
from jax.experimental import pallas as pl
from jax.experimental.pallas import tpu as pltpu
from jax.sharding import PartitionSpec as P

HEAD = 128


def from_behind(block, axis, distance):
    devices = range(lax.axis_size(axis))
    route = [(i - distance, i) for i in devices if i - distance in devices]
    return lax.ppermute(block, axis, route)


def trailing_softmax(scores):
    top = jnp.max(scores, axis=-1, keepdims=True)
    expo = jnp.exp(scores - top)
    return expo / jnp.sum(expo, axis=-1, keepdims=True)


def add_rows(left, piece):
    return jnp.dot(left, piece, preferred_element_type=jnp.float32)


def shards(tokens, key_weight, query_weight, latent_queries, init_memory, forget):
    local = tokens[0]
    width = local.shape[1]
    heads = width // HEAD
    latents = latent_queries.shape[0]
    whole = lax.all_gather(local, "tp", axis=1, tiled=True)

    def add_one(piece):
        return add_rows(whole, piece)

    keys_full = add_one(lax.all_gather(key_weight, "vid", axis=0, tiled=True))
    queries_full = add_one(lax.all_gather(query_weight, "vid", axis=0, tiled=True))
    scale = 1.0 / jnp.sqrt(jnp.float32(HEAD))
    keys = keys_full.astype(jnp.bfloat16).reshape(-1, heads, HEAD)
    queries = queries_full.astype(jnp.bfloat16).reshape(-1, heads, HEAD)
    values = local.reshape(-1, heads, HEAD)
    latent = latent_queries.reshape(latents, heads, HEAD)
    scores = jnp.einsum("mhe,the->hmt", latent, keys, preferred_element_type=jnp.float32) * scale
    weight_params = trailing_softmax(scores).astype(jnp.bfloat16)
    update = jnp.einsum(
        "hmt,the->mhe", weight_params, values, preferred_element_type=jnp.float32
    ).reshape(latents, width)
    retain = forget[0]
    initial_memory = init_memory[0]
    first = lax.axis_index("seg") == 0

    def turn(step, memory_now):
        received = from_behind(retain * memory_now + update, "seg", 1)
        return jnp.where(first, initial_memory, received)

    memory_in = lax.fori_loop(0, lax.axis_size("seg") - 1, turn, initial_memory)
    memory_out = retain * memory_in + update
    grouped = memory_in.reshape(latents, heads, HEAD)
    normed = grouped * lax.rsqrt(jnp.mean(grouped * grouped, axis=-1, keepdims=True) + 1e-06)
    read_scores = (
        jnp.einsum(
            "the,mhe->htm", queries, normed.astype(jnp.bfloat16), preferred_element_type=jnp.float32
        )
        * scale
    )
    read_weights = trailing_softmax(read_scores).astype(jnp.bfloat16)
    read = jnp.einsum(
        "htm,mhe->the",
        read_weights,
        grouped.astype(jnp.bfloat16),
        preferred_element_type=jnp.float32,
    )
    mixed = (local.astype(jnp.float32) + read.reshape(-1, width)).astype(jnp.bfloat16)
    return (mixed[None], memory_out[None])


CORES = 2
TILE = 2 * HEAD
AHEAD = 4
BEHIND = 2


def softmax_rows(scores):
    top = jnp.max(scores, axis=-1, keepdims=True)
    expo = jnp.exp(scores - top)
    return (expo * (1.0 / jnp.sum(expo, axis=-1, keepdims=True))).astype(jnp.bfloat16)


def fused_kernel(
    segs, vids, tps,
    tokens, key_w, query_w, latent_in, init_memory, forget_in,
    mixed, memory_out,
    weights, tok, queries, memory_in, update, partial, latent, forget,
    load_sem, tok_send, tok_recv, z_send, z_recv, y_send, y_recv, d_send, d_recv, m_send, m_recv,
):
    s, z, t = lax.axis_index("seg"), lax.axis_index("vid"), lax.axis_index("tp")
    y, core = s // CORES, s % CORES
    partner = y * CORES + (1 - core)
    across = (1 - y) * CORES + core
    count, width = tokens.shape
    tiles = width // TILE
    blocks = vids // tps
    depth = blocks * weights.shape[2] * weights.shape[3]
    chunks = range(2 * tiles)
    sides = (1, -1)

    def remote(src, dst, send, recv, device):
        return pltpu.make_async_remote_copy(
            src_ref=src, dst_ref=dst, send_sem=send, recv_sem=recv,
            device_id=device, device_id_type=pl.DeviceIdType.MESH,
        )

    def tile_cols(k):
        return pl.ds(k % tiles * TILE, TILE)

    def z_copy(k, source, side):
        block = weights.at[k, source, s]
        return remote(block, block, z_send.at[k, source, (1 - side) // 2], z_recv.at[k, source], {"vid": z + side})

    def y_copy(k, source, owner):
        block = weights.at[k, source, owner]
        return remote(block, block, y_send.at[k, source], y_recv.at[k, source], {"seg": across})

    def d_copy(k, source, owner, kind):
        block = weights.at[k, source, owner]
        return remote(block, block, d_send.at[k, source, kind], d_recv.at[k, source, kind], {"seg": partner})

    def m_copy(c, device):
        cols = tile_cols(c)
        return remote(memory_out.at[:, cols], memory_in.at[:, cols], m_send.at[c], m_recv.at[c], {"seg": device})

    def inside(index, size):
        return (index >= 0) & (index < size)

    def flag(condition):
        return jnp.where(condition, 1, 0).astype(jnp.int32)

    loads = [
        pltpu.make_async_copy(
            (key_w, query_w)[k // tiles].at[:, :, tile_cols(k)], weights.at[k, z], load_sem.at[k]
        )
        for k in chunks
    ]
    tok_load = pltpu.make_async_copy(tokens, tok.at[t], load_sem.at[len(loads)])
    first_memory = pltpu.make_async_copy(init_memory, memory_in, load_sem.at[len(loads) + 1])
    latent_load = pltpu.make_async_copy(latent_in, latent, load_sem.at[len(loads) + 2])
    forget_load = pltpu.make_async_copy(forget_in, forget, load_sem.at[len(loads) + 3])
    for load in loads[:1] + [tok_load] + loads[1:] + [latent_load, forget_load]:
        load.start()

    @pl.when(s == 0)
    def _():
        first_memory.start()

    barrier = pltpu.get_barrier_semaphore()
    greeted = [
        (z + 1 < vids, {"vid": z + 1}),
        (z > 0, {"vid": z - 1}),
        (s >= 0, {"seg": across}),
        ((core == 1) & (y == 0), {"seg": s + 1}),
        ((core == 0) & (y == 1), {"seg": s - 1}),
        (s >= 0, {"seg": partner}),
        (s >= 0, {"tp": 1 - t}),
    ]
    waited = 0
    for condition, device in greeted:
        waited = waited + flag(condition)

        @pl.when(condition)
        def _(device=device):
            pl.semaphore_signal(barrier, inc=1, device_id=device, device_id_type=pl.DeviceIdType.MESH)

    pl.semaphore_wait(barrier, waited)

    def own_sends(k):
        for side in sides:
            @pl.when(inside(z + side, vids))
            def _(side=side):
                z_copy(k, z, side).start()

    tok_copy = remote(tok.at[t], tok.at[t], tok_send, tok_recv, {"tp": 1 - t})
    for k in chunks[:AHEAD]:
        loads[k].wait()
        own_sends(k)
        if k == 0:
            tok_load.wait()
            tok_copy.start()
    for k in chunks[AHEAD:]:
        loads[k].wait()
    latent_load.wait()
    forget_load.wait()

    @pl.when(s == 0)
    def _():
        first_memory.wait()

    def each_source(distance, action):
        for side in sides:
            source = z - side * distance

            @pl.when(inside(source, vids))
            def _(source=source, side=side):
                action(source, side)

    def arrive_z(k, distance):
        def action(source, side):
            z_copy(k, source, side).wait_recv()

            @pl.when(inside(z + side, vids))
            def _():
                z_copy(k, source, side).start()

            y_copy(k, source, s).start()
            d_copy(k, source, s, 0).start()

        each_source(distance, action)
        if distance == vids - 1 and k + AHEAD < len(chunks):
            own_sends(k + AHEAD)

    def arrive_y(k, distance):
        def action(source, side):
            y_copy(k, source, across).wait_recv()
            d_copy(k, source, across, 1).start()

        each_source(distance, action)

    def arrive_d(k):
        for distance in range(1, vids):
            def action(source, side):
                d_copy(k, source, partner, 0).wait_recv()
                d_copy(k, source, (1 - y) * CORES + 1 - core, 1).wait_recv()

            each_source(distance, action)

    def half_product(k, half):
        right = weights[k, pl.ds(half * blocks, blocks)].reshape(depth, TILE)
        return jnp.dot(tok[half], right, preferred_element_type=jnp.float32)

    scale = 1.0 / jnp.sqrt(jnp.float32(HEAD))

    def key_near(k):
        arrive_d(k)
        partial[k] = half_product(k, t)

    def key_far(k):
        keys = (partial[k] + half_product(k, 1 - t)).astype(jnp.bfloat16)
        for h in range(TILE // HEAD):
            cols = pl.ds(k * TILE + h * HEAD, HEAD)
            scores = lax.dot_general(
                latent[:, cols], keys[:, h * HEAD:(h + 1) * HEAD], (((1,), (1,)), ((), ())),
                preferred_element_type=jnp.float32,
            )
            update[:, cols] = jnp.dot(softmax_rows(scores * scale), tok[t, :, cols], preferred_element_type=jnp.float32)

    def carry(c, seg):
        cols = tile_cols(c)

        @pl.when(s == seg)
        def _():
            if seg > 0:
                m_copy(c, s - 1).wait_recv()
            memory_out[:, cols] = forget[:, cols] * memory_in[:, cols] + update[:, cols]
            if seg + 1 < segs:
                m_copy(c, s + 1).start()

    def query(k):
        arrive_d(k)
        queries[:, tile_cols(k)] = (half_product(k, t) + half_product(k, 1 - t)).astype(jnp.bfloat16)

    def readout(k):
        for h in range(TILE // HEAD):
            cols = pl.ds(k % tiles * TILE + h * HEAD, HEAD)
            held = memory_in[:, cols]
            normed = held * lax.rsqrt(jnp.mean(held * held, axis=-1, keepdims=True) + 1e-06)
            scores = lax.dot_general(
                queries[:, cols], normed.astype(jnp.bfloat16), (((1,), (1,)), ((), ())),
                preferred_element_type=jnp.float32,
            )
            read = jnp.dot(softmax_rows(scores * scale), held.astype(jnp.bfloat16), preferred_element_type=jnp.float32)
            mixed[:, cols] = (tok[t, :, cols].astype(jnp.float32) + read).astype(jnp.bfloat16)

    def far_tokens():
        remote(tok.at[1 - t], tok.at[1 - t], tok_send, tok_recv, {"tp": 1 - t}).wait_recv()

    gaps = vids - 1
    slots = [(k, distance) for k in chunks for distance in range(1, vids)]
    tasks = {}

    def place(slot, task, *args):
        tasks.setdefault(min(slot, len(slots) + BEHIND), []).append((task, args))

    done = [gaps * k + gaps - 1 + BEHIND + 1 for k in chunks]
    for k in range(tiles):
        place(done[k], key_near, k)
    start = done[tiles - 1]
    place(start, far_tokens)
    for k in range(tiles):
        place(start + k, key_far, k)
        for seg, lag in enumerate((0, 1, 4, 5)):
            place(start + k + lag, carry, k, seg)
    for k in range(tiles, 2 * tiles):
        place(done[k], query, k)
    for k in range(tiles, 2 * tiles):
        place(max(done[k], start + k - tiles + 6), readout, k)

    for at in range(len(slots) + BEHIND + 1):
        if at < len(slots):
            arrive_z(*slots[at])
        if 0 <= at - BEHIND < len(slots):
            arrive_y(*slots[at - BEHIND])
        for task, args in tasks.get(at, []):
            task(*args)

    tok_copy.wait_send()
    for k in chunks:
        for side in sides:
            @pl.when(inside(z + side, vids))
            def _(k=k, side=side):
                z_copy(k, z, side).wait_send()

        for distance in range(1, vids):
            def sent(source, side, k=k):
                @pl.when(inside(z + side, vids))
                def _():
                    z_copy(k, source, side).wait_send()

                y_copy(k, source, s).wait_send()
                d_copy(k, source, s, 0).wait_send()
                d_copy(k, source, across, 1).wait_send()

            each_source(distance, sent)

    @pl.when(s + 1 < segs)
    def _():
        for c in range(tiles):
            m_copy(c, s + 1).wait_send()


def fused_shards(sizes, tokens, key_weight, query_weight, latent_queries, init_memory, forget):
    segs, vids, tps = sizes
    local = tokens[0]
    count, width = local.shape
    latents = latent_queries.shape[0]
    rows = key_weight.shape[0]
    tiles = width // TILE
    parts = (segs, rows // segs, width)
    hbm = pl.BlockSpec(memory_space=pltpu.HBM)
    vmem = pl.BlockSpec(memory_space=pltpu.VMEM)
    dma = pltpu.SemaphoreType.DMA
    mixed, memory = pl.pallas_call(
        functools.partial(fused_kernel, segs, vids, tps),
        out_shape=(
            jax.ShapeDtypeStruct((count, width), jnp.bfloat16),
            jax.ShapeDtypeStruct((latents, width), jnp.float32),
        ),
        in_specs=[hbm] * 6,
        out_specs=(vmem, vmem),
        scratch_shapes=[
            pltpu.VMEM((2 * tiles, vids, segs, rows // segs, TILE), jnp.bfloat16),
            pltpu.VMEM((tps, count, width), jnp.bfloat16),
            pltpu.VMEM((count, width), jnp.bfloat16),
            pltpu.VMEM((latents, width), jnp.float32),
            pltpu.VMEM((latents, width), jnp.float32),
            pltpu.VMEM((tiles, count, TILE), jnp.float32),
            pltpu.VMEM((latents, width), jnp.bfloat16),
            pltpu.VMEM((1, width), jnp.float32),
            dma((2 * tiles + 4,)),
            dma,
            dma,
            dma((2 * tiles, vids, 2)),
            dma((2 * tiles, vids)),
            dma((2 * tiles, vids)),
            dma((2 * tiles, vids)),
            dma((2 * tiles, vids, 2)),
            dma((2 * tiles, vids, 2)),
            dma((tiles,)),
            dma((tiles,)),
        ],
        compiler_params=pltpu.CompilerParams(
            collective_id=0, has_side_effects=True, vmem_limit_bytes=GRANT
        ),
    )(
        *(
            pltpu.with_memory_space_constraint(array, pltpu.HBM)
            for array in (
                local, key_weight.reshape(parts), query_weight.reshape(parts), latent_queries, init_memory[0], forget[0]
            )
        )
    )
    return (mixed[None], memory[None])


GRANT = 28 * 1024 * 1024


def relay_fits(segs, vids, tps):
    return tps == 2 and segs == 2 * CORES and vids > 2 and vids % tps == 0 and segs * vids <= 32


def solution(mesh):
    placed = (
        P("vid", "seg", "tp"),
        P("vid", "tp"),
        P("vid", "tp"),
        P(None, "tp"),
        P("vid", None, "tp"),
        P("vid", "seg", "tp"),
    )
    sizes = tuple(mesh.shape[axis] for axis in ("seg", "vid", "tp"))
    body = functools.partial(fused_shards, sizes) if relay_fits(*sizes) else shards
    return jax.shard_map(
        body,
        mesh=mesh,
        in_specs=placed,
        out_specs=(P("vid", "seg", "tp"), P("vid", "seg", "tp")),
        check_vma=False,
    )
```

```python
import functools

import jax
import jax.numpy as jnp
from jax import lax
from jax.experimental import pallas as pl
from jax.experimental.pallas import tpu as pltpu
from jax.sharding import PartitionSpec as P

HEAD = 128


def from_behind(block, axis, distance):
    devices = range(lax.axis_size(axis))
    route = [(i - distance, i) for i in devices if i - distance in devices]
    return lax.ppermute(block, axis, route)


def trailing_softmax(scores):
    top = jnp.max(scores, axis=-1, keepdims=True)
    expo = jnp.exp(scores - top)
    return expo / jnp.sum(expo, axis=-1, keepdims=True)


def add_rows(left, piece):
    return jnp.dot(left, piece, preferred_element_type=jnp.float32)


def shards(tokens, key_weight, query_weight, latent_queries, init_memory, forget):
    local = tokens[0]
    width = local.shape[1]
    heads = width // HEAD
    latents = latent_queries.shape[0]
    whole = lax.all_gather(local, "tp", axis=1, tiled=True)

    def add_one(piece):
        return add_rows(whole, piece)

    keys_full = add_one(lax.all_gather(key_weight, "vid", axis=0, tiled=True))
    queries_full = add_one(lax.all_gather(query_weight, "vid", axis=0, tiled=True))
    scale = 1.0 / jnp.sqrt(jnp.float32(HEAD))
    keys = keys_full.astype(jnp.bfloat16).reshape(-1, heads, HEAD)
    queries = queries_full.astype(jnp.bfloat16).reshape(-1, heads, HEAD)
    values = local.reshape(-1, heads, HEAD)
    latent = latent_queries.reshape(latents, heads, HEAD)
    scores = jnp.einsum("mhe,the->hmt", latent, keys, preferred_element_type=jnp.float32) * scale
    weight_params = trailing_softmax(scores).astype(jnp.bfloat16)
    update = jnp.einsum(
        "hmt,the->mhe", weight_params, values, preferred_element_type=jnp.float32
    ).reshape(latents, width)
    retain = forget[0]
    initial_memory = init_memory[0]
    first = lax.axis_index("seg") == 0

    def turn(step, memory_now):
        received = from_behind(retain * memory_now + update, "seg", 1)
        return jnp.where(first, initial_memory, received)

    memory_in = lax.fori_loop(0, lax.axis_size("seg") - 1, turn, initial_memory)
    memory_out = retain * memory_in + update
    grouped = memory_in.reshape(latents, heads, HEAD)
    normed = grouped * lax.rsqrt(jnp.mean(grouped * grouped, axis=-1, keepdims=True) + 1e-06)
    read_scores = (
        jnp.einsum(
            "the,mhe->htm", queries, normed.astype(jnp.bfloat16), preferred_element_type=jnp.float32
        )
        * scale
    )
    read_weights = trailing_softmax(read_scores).astype(jnp.bfloat16)
    read = jnp.einsum(
        "htm,mhe->the",
        read_weights,
        grouped.astype(jnp.bfloat16),
        preferred_element_type=jnp.float32,
    )
    mixed = (local.astype(jnp.float32) + read.reshape(-1, width)).astype(jnp.bfloat16)
    return (mixed[None], memory_out[None])


CORES = 2
TILE = 2 * HEAD
AHEAD = 3
SKEW = 1
HOLD = 0
BEHIND = 4
LATE = 4
DIRECT = 1
EARLY = 1
STEP = 0
LAGS = (0, 1, 8, 9)
GROUP = 4


def softmax_rows(scores):
    top = jnp.max(scores, axis=-1, keepdims=True)
    expo = jnp.exp(scores - top)
    return (expo * (1.0 / jnp.sum(expo, axis=-1, keepdims=True))).astype(jnp.bfloat16)


def fused_kernel(
    segs, vids, tps,
    tokens, key_w, query_w, latent_in, init_memory, forget_in,
    mixed, memory_out,
    weights, tok, queries, memory_in, update, partial, raised, flipped, latent, forget,
    load_sem, tok_send, tok_recv, z_send, z_recv, y_send, y_recv, d_send, d_recv, m_send, m_recv,
):
    s, z, t = lax.axis_index("seg"), lax.axis_index("vid"), lax.axis_index("tp")
    y, core = s // CORES, s % CORES
    partner = y * CORES + (1 - core)
    across = (1 - y) * CORES + core
    count, width = tokens.shape
    tiles = width // TILE
    blocks = vids // tps
    depth = blocks * weights.shape[2] * weights.shape[3]
    chunks = range(2 * tiles)
    sides = (1, -1)

    def remote(src, dst, send, recv, device):
        return pltpu.make_async_remote_copy(
            src_ref=src, dst_ref=dst, send_sem=send, recv_sem=recv,
            device_id=device, device_id_type=pl.DeviceIdType.MESH,
        )

    def tile_cols(k):
        return pl.ds(k % tiles * TILE, TILE)

    def lanes(k):
        return (s, across) if k >= len(chunks) - DIRECT else (s,)

    def z_copy(k, source, side, lane):
        block = weights.at[k, source, lanes(k)[lane]]
        return remote(
            block, block, z_send.at[k, source, (1 - side) // 2, lane], z_recv.at[k, source, lane], {"vid": z + side}
        )

    def y_copy(k, source, owner):
        block = weights.at[k, source, owner]
        return remote(block, block, y_send.at[k, source], y_recv.at[k, source], {"seg": across})

    def d_copy(k, source, owner, kind):
        block = weights.at[k, source, owner]
        return remote(block, block, d_send.at[k, source, kind], d_recv.at[k, source, kind], {"seg": partner})

    def m_copy(c, device):
        cols = tile_cols(c)
        return remote(memory_out.at[:, cols], memory_in.at[:, cols], m_send.at[c], m_recv.at[c], {"seg": device})

    def inside(index, size):
        return (index >= 0) & (index < size)

    def flag(condition):
        return jnp.where(condition, 1, 0).astype(jnp.int32)

    loads = [
        pltpu.make_async_copy(
            (key_w, query_w)[k // tiles].at[:, :, tile_cols(k)], weights.at[k, z], load_sem.at[k]
        )
        for k in chunks
    ]
    tok_load = pltpu.make_async_copy(tokens, tok.at[t], load_sem.at[len(loads)])
    first_memory = pltpu.make_async_copy(init_memory, memory_in, load_sem.at[len(loads) + 1])
    latent_load = pltpu.make_async_copy(latent_in, latent, load_sem.at[len(loads) + 2])
    forget_load = pltpu.make_async_copy(forget_in, forget, load_sem.at[len(loads) + 3])
    for load in loads[:1] + [tok_load] + loads[1:] + [latent_load, forget_load]:
        load.start()

    @pl.when(s == 0)
    def _():
        first_memory.start()

    barrier = pltpu.get_barrier_semaphore()
    greeted = [
        (z + 1 < vids, {"vid": z + 1}),
        (z > 0, {"vid": z - 1}),
        (s >= 0, {"seg": across}),
        ((core == 1) & (y == 0), {"seg": s + 1}),
        ((core == 0) & (y == 1), {"seg": s - 1}),
        (s >= 0, {"seg": partner}),
        (s >= 0, {"tp": 1 - t}),
    ]
    waited = 0
    for condition, device in greeted:
        waited = waited + flag(condition)

        @pl.when(condition)
        def _(device=device):
            pl.semaphore_signal(barrier, inc=1, device_id=device, device_id_type=pl.DeviceIdType.MESH)

    pl.semaphore_wait(barrier, waited)

    def own_sends(k):
        for side in sides:
            @pl.when(inside(z + side, vids))
            def _(side=side):
                for lane in range(len(lanes(k))):
                    z_copy(k, z, side, lane).start()

    tok_copy = remote(tok.at[t], tok.at[t], tok_send, tok_recv, {"tp": 1 - t})
    for k in chunks[:AHEAD]:
        loads[k].wait()
        own_sends(k)
        if k == 0:
            tok_load.wait()
            tok_copy.start()
    for k in chunks[AHEAD:]:
        loads[k].wait()
    latent_load.wait()
    forget_load.wait()

    @pl.when(s == 0)
    def _():
        first_memory.wait()

    def each_source(distance, action):
        for side in sides:
            source = z - side * distance

            @pl.when(inside(source, vids))
            def _(source=source, side=side):
                action(source, side)

    def arrive_z(k, distance):
        def action(source, side):
            for lane, owner in enumerate(lanes(k)):
                z_copy(k, source, side, lane).wait_recv()

                @pl.when(inside(z + side, vids))
                def _(lane=lane):
                    z_copy(k, source, side, lane).start()

                if len(lanes(k)) == 1:
                    y_copy(k, source, owner).start()
                d_copy(k, source, owner, lane).start()

        each_source(distance, action)
        if distance == 1 and k + AHEAD < len(chunks):
            own_sends(k + AHEAD)

    def arrive_y(k, distance):
        def action(source, side):
            y_copy(k, source, across).wait_recv()
            d_copy(k, source, across, 1).start()

        if len(lanes(k)) == 1:
            each_source(distance, action)

    def arrive_d(k):
        for distance in range(1, vids):
            def action(source, side):
                d_copy(k, source, partner, 0).wait_recv()
                d_copy(k, source, (1 - y) * CORES + 1 - core, 1).wait_recv()

            each_source(distance, action)

    def half_product(k, half):
        right = weights[k, pl.ds(half * blocks, blocks)].reshape(depth, TILE)
        return jnp.dot(tok[half], right, preferred_element_type=jnp.float32)

    scale = 1.0 / jnp.sqrt(jnp.float32(HEAD))

    def flip(k):
        flipped[tile_cols(k)] = tok[t, :, tile_cols(k)].T

    def key_near(k):
        arrive_d(k)
        partial[k] = half_product(k, t)

    def key_far(k):
        keys = (partial[k] + half_product(k, 1 - t)).astype(jnp.bfloat16)
        for h in range(TILE // HEAD):
            cols = pl.ds(k * TILE + h * HEAD, HEAD)
            raised[:, cols] = lax.dot_general(
                keys[:, h * HEAD:(h + 1) * HEAD], latent[:, cols], (((1,), (1,)), ((), ())),
                preferred_element_type=jnp.float32,
            ) * scale

    def blend(group):
        at = group[0] * TILE
        span = len(group) * TILE
        scores = raised[:, at:at + span]
        expo = jnp.exp(scores - jnp.max(scores, axis=0, keepdims=True))
        held = (expo * (1.0 / jnp.sum(expo, axis=0, keepdims=True))).astype(jnp.bfloat16)
        for h in range(span // HEAD):
            cols = pl.ds(at + h * HEAD, HEAD)
            update[:, cols] = jnp.dot(
                flipped[cols], held[:, h * HEAD:(h + 1) * HEAD], preferred_element_type=jnp.float32
            ).T

    def carry(c, seg):
        cols = tile_cols(c)

        @pl.when(s == seg)
        def _():
            if seg > 0:
                m_copy(c, s - 1).wait_recv()
            memory_out[:, cols] = forget[:, cols] * memory_in[:, cols] + update[:, cols]
            if seg + 1 < segs:
                m_copy(c, s + 1).start()

    def query(k):
        arrive_d(k)
        queries[:, tile_cols(k)] = (half_product(k, t) + half_product(k, 1 - t)).astype(jnp.bfloat16)

    def readout(k):
        for h in range(TILE // HEAD):
            cols = pl.ds(k % tiles * TILE + h * HEAD, HEAD)
            held = memory_in[:, cols]
            normed = held * lax.rsqrt(jnp.mean(held * held, axis=-1, keepdims=True) + 1e-06)
            scores = lax.dot_general(
                queries[:, cols], normed.astype(jnp.bfloat16), (((1,), (1,)), ((), ())),
                preferred_element_type=jnp.float32,
            )
            read = jnp.dot(softmax_rows(scores * scale), held.astype(jnp.bfloat16), preferred_element_type=jnp.float32)
            mixed[:, cols] = (tok[t, :, cols].astype(jnp.float32) + read).astype(jnp.bfloat16)

    def far_tokens():
        remote(tok.at[1 - t], tok.at[1 - t], tok_send, tok_recv, {"tp": 1 - t}).wait_recv()

    gaps = vids - 1
    slots = [(k, distance) for k in chunks for distance in range(1, vids)]
    slots.sort(key=lambda slot: (slot[0] + SKEW * (slot[1] - 1) + HOLD * (slot[0] >= tiles), slot[1]))
    relays = [
        (at + (BEHIND if slot[0] < tiles else LATE), slot) for at, slot in enumerate(slots) if len(lanes(slot[0])) == 1
    ]
    done = {k: slots.index((k, gaps)) + 1 for k in chunks}
    for at, (k, _) in relays:
        done[k] = max(done[k], at + 1)
    plan = []

    def place(at, task, *args):
        plan.append((at, task, args))

    start = done[tiles - 1] - EARLY
    for k in range(tiles):
        place(k + 1, flip, k)
        place(done[k], key_near, k)
    place(start, far_tokens)
    for k in range(tiles):
        place(max(start, done[k]) + STEP * k, key_far, k)
    mixed_at = max(start, done[tiles - 1]) + STEP * (tiles - 1)
    for at in range(0, tiles, GROUP):
        place(mixed_at, blend, range(at, min(at + GROUP, tiles)))
    for k in range(tiles):
        for seg, lag in enumerate(LAGS):
            place(mixed_at + lag, carry, k, seg)
    for k in range(tiles, 2 * tiles):
        place(done[k], query, k)
        place(max(done[k], mixed_at + LAGS[-1]), readout, k)
    for at, slot in enumerate(slots):
        place(at - 0.2, arrive_z, *slot)
    for at, slot in relays:
        place(at - 0.1, arrive_y, *slot)
    for at, task, args in sorted(plan, key=lambda entry: entry[0]):
        task(*args)

    tok_copy.wait_send()
    for k in chunks:
        for side in sides:
            @pl.when(inside(z + side, vids))
            def _(k=k, side=side):
                for lane in range(len(lanes(k))):
                    z_copy(k, z, side, lane).wait_send()

        for distance in range(1, vids):
            def sent(source, side, k=k):
                @pl.when(inside(z + side, vids))
                def _():
                    for lane in range(len(lanes(k))):
                        z_copy(k, source, side, lane).wait_send()

                if len(lanes(k)) == 1:
                    y_copy(k, source, s).wait_send()
                d_copy(k, source, s, 0).wait_send()
                d_copy(k, source, across, 1).wait_send()

            each_source(distance, sent)

    @pl.when(s + 1 < segs)
    def _():
        for c in range(tiles):
            m_copy(c, s + 1).wait_send()


def fused_shards(sizes, tokens, key_weight, query_weight, latent_queries, init_memory, forget):
    segs, vids, tps = sizes
    local = tokens[0]
    count, width = local.shape
    latents = latent_queries.shape[0]
    rows = key_weight.shape[0]
    tiles = width // TILE
    parts = (segs, rows // segs, width)
    hbm = pl.BlockSpec(memory_space=pltpu.HBM)
    vmem = pl.BlockSpec(memory_space=pltpu.VMEM)
    dma = pltpu.SemaphoreType.DMA
    mixed, memory = pl.pallas_call(
        functools.partial(fused_kernel, segs, vids, tps),
        out_shape=(
            jax.ShapeDtypeStruct((count, width), jnp.bfloat16),
            jax.ShapeDtypeStruct((latents, width), jnp.float32),
        ),
        in_specs=[hbm] * 6,
        out_specs=(vmem, vmem),
        scratch_shapes=[
            pltpu.VMEM((2 * tiles, vids, segs, rows // segs, TILE), jnp.bfloat16),
            pltpu.VMEM((tps, count, width), jnp.bfloat16),
            pltpu.VMEM((count, width), jnp.bfloat16),
            pltpu.VMEM((latents, width), jnp.float32),
            pltpu.VMEM((latents, width), jnp.float32),
            pltpu.VMEM((tiles, count, TILE), jnp.float32),
            pltpu.VMEM((count, width), jnp.float32),
            pltpu.VMEM((width, count), jnp.bfloat16),
            pltpu.VMEM((latents, width), jnp.bfloat16),
            pltpu.VMEM((1, width), jnp.float32),
            dma((2 * tiles + 4,)),
            dma,
            dma,
            dma((2 * tiles, vids, 2, 2)),
            dma((2 * tiles, vids, 2)),
            dma((2 * tiles, vids)),
            dma((2 * tiles, vids)),
            dma((2 * tiles, vids, 2)),
            dma((2 * tiles, vids, 2)),
            dma((tiles,)),
            dma((tiles,)),
        ],
        compiler_params=pltpu.CompilerParams(
            collective_id=0, has_side_effects=True, vmem_limit_bytes=GRANT
        ),
    )(
        *(
            pltpu.with_memory_space_constraint(array, pltpu.HBM)
            for array in (
                local, key_weight.reshape(parts), query_weight.reshape(parts), latent_queries, init_memory[0], forget[0]
            )
        )
    )
    return (mixed[None], memory[None])


GRANT = 28 * 1024 * 1024


def relay_fits(segs, vids, tps):
    return tps == 2 and segs == 2 * CORES and vids > 2 and vids % tps == 0 and segs * vids <= 32


def solution(mesh):
    placed = (
        P("vid", "seg", "tp"),
        P("vid", "tp"),
        P("vid", "tp"),
        P(None, "tp"),
        P("vid", None, "tp"),
        P("vid", "seg", "tp"),
    )
    sizes = tuple(mesh.shape[axis] for axis in ("seg", "vid", "tp"))
    body = functools.partial(fused_shards, sizes) if relay_fits(*sizes) else shards
    return jax.shard_map(
        body,
        mesh=mesh,
        in_specs=placed,
        out_specs=(P("vid", "seg", "tp"), P("vid", "seg", "tp")),
        check_vma=False,
    )
```

```python
import functools

import jax
import jax.numpy as jnp
from jax import lax
from jax.experimental import pallas as pl
from jax.experimental.pallas import tpu as pltpu
from jax.sharding import PartitionSpec as P

HEAD = 128


def from_behind(block, axis, distance):
    devices = range(lax.axis_size(axis))
    route = [(i - distance, i) for i in devices if i - distance in devices]
    return lax.ppermute(block, axis, route)


def trailing_softmax(scores):
    top = jnp.max(scores, axis=-1, keepdims=True)
    expo = jnp.exp(scores - top)
    return expo / jnp.sum(expo, axis=-1, keepdims=True)


def add_rows(left, piece):
    return jnp.dot(left, piece, preferred_element_type=jnp.float32)


def shards(tokens, key_weight, query_weight, latent_queries, init_memory, forget):
    local = tokens[0]
    width = local.shape[1]
    heads = width // HEAD
    latents = latent_queries.shape[0]
    whole = lax.all_gather(local, "tp", axis=1, tiled=True)

    def add_one(piece):
        return add_rows(whole, piece)

    keys_full = add_one(lax.all_gather(key_weight, "vid", axis=0, tiled=True))
    queries_full = add_one(lax.all_gather(query_weight, "vid", axis=0, tiled=True))
    scale = 1.0 / jnp.sqrt(jnp.float32(HEAD))
    keys = keys_full.astype(jnp.bfloat16).reshape(-1, heads, HEAD)
    queries = queries_full.astype(jnp.bfloat16).reshape(-1, heads, HEAD)
    values = local.reshape(-1, heads, HEAD)
    latent = latent_queries.reshape(latents, heads, HEAD)
    scores = jnp.einsum("mhe,the->hmt", latent, keys, preferred_element_type=jnp.float32) * scale
    weight_params = trailing_softmax(scores).astype(jnp.bfloat16)
    update = jnp.einsum(
        "hmt,the->mhe", weight_params, values, preferred_element_type=jnp.float32
    ).reshape(latents, width)
    retain = forget[0]
    initial_memory = init_memory[0]
    first = lax.axis_index("seg") == 0

    def turn(step, memory_now):
        received = from_behind(retain * memory_now + update, "seg", 1)
        return jnp.where(first, initial_memory, received)

    memory_in = lax.fori_loop(0, lax.axis_size("seg") - 1, turn, initial_memory)
    memory_out = retain * memory_in + update
    grouped = memory_in.reshape(latents, heads, HEAD)
    normed = grouped * lax.rsqrt(jnp.mean(grouped * grouped, axis=-1, keepdims=True) + 1e-06)
    read_scores = (
        jnp.einsum(
            "the,mhe->htm", queries, normed.astype(jnp.bfloat16), preferred_element_type=jnp.float32
        )
        * scale
    )
    read_weights = trailing_softmax(read_scores).astype(jnp.bfloat16)
    read = jnp.einsum(
        "htm,mhe->the",
        read_weights,
        grouped.astype(jnp.bfloat16),
        preferred_element_type=jnp.float32,
    )
    mixed = (local.astype(jnp.float32) + read.reshape(-1, width)).astype(jnp.bfloat16)
    return (mixed[None], memory_out[None])


CORES = 2
TILE = 2 * HEAD
AHEAD = 3
SKEW = 1
HOLD = 0
BEHIND = 4
LATE = 4
DIRECT = 2
EARLY = 1
STEP = 0
LAGS = (0, 1, 6, 7)
GROUP = 4


def softmax_rows(scores):
    top = jnp.max(scores, axis=-1, keepdims=True)
    expo = jnp.exp(scores - top)
    return (expo * (1.0 / jnp.sum(expo, axis=-1, keepdims=True))).astype(jnp.bfloat16)


def fused_kernel(
    segs, vids, tps,
    tokens, key_w, query_w, latent_in, init_memory, forget_in,
    mixed, memory_out,
    weights, tok, queries, memory_in, update, partial, raised, flipped, latent, forget,
    load_sem, tok_send, tok_recv, z_send, z_recv, y_send, y_recv, d_send, d_recv, m_send, m_recv,
):
    s, z, t = lax.axis_index("seg"), lax.axis_index("vid"), lax.axis_index("tp")
    y, core = s // CORES, s % CORES
    partner = y * CORES + (1 - core)
    across = (1 - y) * CORES + core
    count, width = tokens.shape
    tiles = width // TILE
    blocks = vids // tps
    depth = blocks * weights.shape[2] * weights.shape[3]
    chunks = range(2 * tiles)
    sides = (1, -1)

    def remote(src, dst, send, recv, device):
        return pltpu.make_async_remote_copy(
            src_ref=src, dst_ref=dst, send_sem=send, recv_sem=recv,
            device_id=device, device_id_type=pl.DeviceIdType.MESH,
        )

    def tile_cols(k):
        return pl.ds(k % tiles * TILE, TILE)

    def lanes(k):
        return (s, across) if k >= len(chunks) - DIRECT else (s,)

    def z_copy(k, source, side, lane):
        block = weights.at[k, source, lanes(k)[lane]]
        return remote(
            block, block, z_send.at[k, source, (1 - side) // 2, lane], z_recv.at[k, source, lane], {"vid": z + side}
        )

    def through(source, side):
        return (vids - 1 - source if side == 1 else source) > 1

    def y_copy(k, source, owner):
        block = weights.at[k, source, owner]
        return remote(block, block, y_send.at[k, source], y_recv.at[k, source], {"seg": across})

    def d_copy(k, source, owner, kind):
        block = weights.at[k, source, owner]
        return remote(block, block, d_send.at[k, source, kind], d_recv.at[k, source, kind], {"seg": partner})

    def m_copy(c, device):
        cols = tile_cols(c)
        return remote(memory_out.at[:, cols], memory_in.at[:, cols], m_send.at[c], m_recv.at[c], {"seg": device})

    def inside(index, size):
        return (index >= 0) & (index < size)

    def flag(condition):
        return jnp.where(condition, 1, 0).astype(jnp.int32)

    loads = [
        pltpu.make_async_copy(
            (key_w, query_w)[k // tiles].at[:, :, tile_cols(k)], weights.at[k, z], load_sem.at[k]
        )
        for k in chunks
    ]
    tok_load = pltpu.make_async_copy(tokens, tok.at[t], load_sem.at[len(loads)])
    first_memory = pltpu.make_async_copy(init_memory, memory_in, load_sem.at[len(loads) + 1])
    latent_load = pltpu.make_async_copy(latent_in, latent, load_sem.at[len(loads) + 2])
    forget_load = pltpu.make_async_copy(forget_in, forget, load_sem.at[len(loads) + 3])
    for load in loads[:1] + [tok_load] + loads[1:] + [latent_load, forget_load]:
        load.start()

    @pl.when(s == 0)
    def _():
        first_memory.start()

    barrier = pltpu.get_barrier_semaphore()
    greeted = [
        (z + 1 < vids, {"vid": z + 1}),
        (z > 0, {"vid": z - 1}),
        (s >= 0, {"seg": across}),
        ((core == 1) & (y == 0), {"seg": s + 1}),
        ((core == 0) & (y == 1), {"seg": s - 1}),
        (s >= 0, {"seg": partner}),
        (s >= 0, {"tp": 1 - t}),
    ]
    waited = 0
    for condition, device in greeted:
        waited = waited + flag(condition)

        @pl.when(condition)
        def _(device=device):
            pl.semaphore_signal(barrier, inc=1, device_id=device, device_id_type=pl.DeviceIdType.MESH)

    pl.semaphore_wait(barrier, waited)

    def own_sends(k):
        for side in sides:
            @pl.when(inside(z + side, vids))
            def _(side=side):
                z_copy(k, z, side, 0).start()

            if len(lanes(k)) > 1:
                @pl.when(inside(z + side, vids) & through(z, side))
                def _(side=side):
                    z_copy(k, z, side, 1).start()

    tok_copy = remote(tok.at[t], tok.at[t], tok_send, tok_recv, {"tp": 1 - t})
    for k in chunks[:AHEAD]:
        loads[k].wait()
        own_sends(k)
        if k == 0:
            tok_load.wait()
            tok_copy.start()
    for k in chunks[AHEAD:]:
        loads[k].wait()
    latent_load.wait()
    forget_load.wait()

    @pl.when(s == 0)
    def _():
        first_memory.wait()

    def each_source(distance, action):
        for side in sides:
            source = z - side * distance

            @pl.when(inside(source, vids))
            def _(source=source, side=side):
                action(source, side)

    def arrive_z(k, distance):
        def action(source, side):
            def take(lane):
                z_copy(k, source, side, lane).wait_recv()

                @pl.when(inside(z + side, vids))
                def _():
                    z_copy(k, source, side, lane).start()

                d_copy(k, source, (s, across)[lane], lane).start()

            take(0)
            if len(lanes(k)) == 1:
                y_copy(k, source, s).start()
            elif distance > 1:
                take(1)
            else:
                @pl.when(through(source, side))
                def _():
                    take(1)

                @pl.when(jnp.logical_not(through(source, side)))
                def _():
                    y_copy(k, source, s).start()

        each_source(distance, action)
        if distance == 1 and k + AHEAD < len(chunks):
            own_sends(k + AHEAD)

    def arrive_y(k, distance):
        def action(source, side):
            def take():
                y_copy(k, source, across).wait_recv()
                d_copy(k, source, across, 1).start()

            if len(lanes(k)) == 1:
                take()
            else:
                pl.when(jnp.logical_not(through(source, side)))(take)

        each_source(distance, action)

    def arrive_d(k):
        for distance in range(1, vids):
            def action(source, side):
                d_copy(k, source, partner, 0).wait_recv()
                d_copy(k, source, (1 - y) * CORES + 1 - core, 1).wait_recv()

            each_source(distance, action)

    def half_product(k, half):
        right = weights[k, pl.ds(half * blocks, blocks)].reshape(depth, TILE)
        return jnp.dot(tok[half], right, preferred_element_type=jnp.float32)

    scale = 1.0 / jnp.sqrt(jnp.float32(HEAD))

    def flip(k):
        flipped[tile_cols(k)] = tok[t, :, tile_cols(k)].T

    def key_near(k):
        arrive_d(k)
        partial[k] = half_product(k, t)

    def key_far(k):
        keys = (partial[k] + half_product(k, 1 - t)).astype(jnp.bfloat16)
        for h in range(TILE // HEAD):
            cols = pl.ds(k * TILE + h * HEAD, HEAD)
            raised[:, cols] = lax.dot_general(
                keys[:, h * HEAD:(h + 1) * HEAD], latent[:, cols], (((1,), (1,)), ((), ())),
                preferred_element_type=jnp.float32,
            ) * scale

    def blend(group):
        at = group[0] * TILE
        span = len(group) * TILE
        scores = raised[:, at:at + span]
        expo = jnp.exp(scores - jnp.max(scores, axis=0, keepdims=True))
        held = (expo * (1.0 / jnp.sum(expo, axis=0, keepdims=True))).astype(jnp.bfloat16)
        for h in range(span // HEAD):
            cols = pl.ds(at + h * HEAD, HEAD)
            update[:, cols] = jnp.dot(
                flipped[cols], held[:, h * HEAD:(h + 1) * HEAD], preferred_element_type=jnp.float32
            ).T

    def carry(c, seg):
        cols = tile_cols(c)

        @pl.when(s == seg)
        def _():
            if seg > 0:
                m_copy(c, s - 1).wait_recv()
            memory_out[:, cols] = forget[:, cols] * memory_in[:, cols] + update[:, cols]
            if seg + 1 < segs:
                m_copy(c, s + 1).start()

    def query(k):
        arrive_d(k)
        queries[:, tile_cols(k)] = (half_product(k, t) + half_product(k, 1 - t)).astype(jnp.bfloat16)

    def readout(k):
        for h in range(TILE // HEAD):
            cols = pl.ds(k % tiles * TILE + h * HEAD, HEAD)
            held = memory_in[:, cols]
            normed = held * lax.rsqrt(jnp.mean(held * held, axis=-1, keepdims=True) + 1e-06)
            scores = lax.dot_general(
                queries[:, cols], normed.astype(jnp.bfloat16), (((1,), (1,)), ((), ())),
                preferred_element_type=jnp.float32,
            )
            read = jnp.dot(softmax_rows(scores * scale), held.astype(jnp.bfloat16), preferred_element_type=jnp.float32)
            mixed[:, cols] = (tok[t, :, cols].astype(jnp.float32) + read).astype(jnp.bfloat16)

    def far_tokens():
        remote(tok.at[1 - t], tok.at[1 - t], tok_send, tok_recv, {"tp": 1 - t}).wait_recv()

    gaps = vids - 1
    slots = [(k, distance) for k in chunks for distance in range(1, vids)]
    slots.sort(key=lambda slot: (slot[0] + SKEW * (slot[1] - 1) + HOLD * (slot[0] >= tiles), slot[1]))
    relays = [
        (at + (BEHIND if slot[0] < tiles else LATE), slot) for at, slot in enumerate(slots)
        if len(lanes(slot[0])) == 1 or slot[1] == 1
    ]
    done = {k: slots.index((k, gaps)) + 1 for k in chunks}
    for at, (k, _) in relays:
        done[k] = max(done[k], at + 1)
    plan = []

    def place(at, task, *args):
        plan.append((at, task, args))

    start = done[tiles - 1] - EARLY
    for k in range(tiles):
        place(k + 1, flip, k)
        place(done[k], key_near, k)
    place(start, far_tokens)
    for k in range(tiles):
        place(max(start, done[k]) + STEP * k, key_far, k)
    mixed_at = max(start, done[tiles - 1]) + STEP * (tiles - 1)
    for at in range(0, tiles, GROUP):
        place(mixed_at, blend, range(at, min(at + GROUP, tiles)))
    for k in range(tiles):
        for seg, lag in enumerate(LAGS):
            place(mixed_at + lag, carry, k, seg)
    for k in range(tiles, 2 * tiles):
        place(done[k], query, k)
        place(max(done[k], mixed_at + LAGS[-1]), readout, k)
    for at, slot in enumerate(slots):
        place(at - 0.2, arrive_z, *slot)
    for at, slot in relays:
        place(at - 0.1, arrive_y, *slot)
    for at, task, args in sorted(plan, key=lambda entry: entry[0]):
        task(*args)

    tok_copy.wait_send()
    for k in chunks:
        for side in sides:
            @pl.when(inside(z + side, vids))
            def _(k=k, side=side):
                z_copy(k, z, side, 0).wait_send()

            if len(lanes(k)) > 1:
                @pl.when(inside(z + side, vids) & through(z, side))
                def _(k=k, side=side):
                    z_copy(k, z, side, 1).wait_send()

        for distance in range(1, vids):
            def sent(source, side, k=k):
                @pl.when(inside(z + side, vids))
                def _():
                    for lane in range(len(lanes(k))):
                        z_copy(k, source, side, lane).wait_send()

                if len(lanes(k)) == 1:
                    y_copy(k, source, s).wait_send()
                elif distance == 1:
                    @pl.when(jnp.logical_not(through(source, side)))
                    def _():
                        y_copy(k, source, s).wait_send()

                d_copy(k, source, s, 0).wait_send()
                d_copy(k, source, across, 1).wait_send()

            each_source(distance, sent)

    @pl.when(s + 1 < segs)
    def _():
        for c in range(tiles):
            m_copy(c, s + 1).wait_send()


def fused_shards(sizes, tokens, key_weight, query_weight, latent_queries, init_memory, forget):
    segs, vids, tps = sizes
    local = tokens[0]
    count, width = local.shape
    latents = latent_queries.shape[0]
    rows = key_weight.shape[0]
    tiles = width // TILE
    parts = (segs, rows // segs, width)
    hbm = pl.BlockSpec(memory_space=pltpu.HBM)
    vmem = pl.BlockSpec(memory_space=pltpu.VMEM)
    dma = pltpu.SemaphoreType.DMA
    mixed, memory = pl.pallas_call(
        functools.partial(fused_kernel, segs, vids, tps),
        out_shape=(
            jax.ShapeDtypeStruct((count, width), jnp.bfloat16),
            jax.ShapeDtypeStruct((latents, width), jnp.float32),
        ),
        in_specs=[hbm] * 6,
        out_specs=(vmem, vmem),
        scratch_shapes=[
            pltpu.VMEM((2 * tiles, vids, segs, rows // segs, TILE), jnp.bfloat16),
            pltpu.VMEM((tps, count, width), jnp.bfloat16),
            pltpu.VMEM((count, width), jnp.bfloat16),
            pltpu.VMEM((latents, width), jnp.float32),
            pltpu.VMEM((latents, width), jnp.float32),
            pltpu.VMEM((tiles, count, TILE), jnp.float32),
            pltpu.VMEM((count, width), jnp.float32),
            pltpu.VMEM((width, count), jnp.bfloat16),
            pltpu.VMEM((latents, width), jnp.bfloat16),
            pltpu.VMEM((1, width), jnp.float32),
            dma((2 * tiles + 4,)),
            dma,
            dma,
            dma((2 * tiles, vids, 2, 2)),
            dma((2 * tiles, vids, 2)),
            dma((2 * tiles, vids)),
            dma((2 * tiles, vids)),
            dma((2 * tiles, vids, 2)),
            dma((2 * tiles, vids, 2)),
            dma((tiles,)),
            dma((tiles,)),
        ],
        compiler_params=pltpu.CompilerParams(
            collective_id=0, has_side_effects=True, vmem_limit_bytes=GRANT
        ),
    )(
        *(
            pltpu.with_memory_space_constraint(array, pltpu.HBM)
            for array in (
                local, key_weight.reshape(parts), query_weight.reshape(parts), latent_queries, init_memory[0], forget[0]
            )
        )
    )
    return (mixed[None], memory[None])


GRANT = 28 * 1024 * 1024


def relay_fits(segs, vids, tps):
    return tps == 2 and segs == 2 * CORES and vids > 2 and vids % tps == 0 and segs * vids <= 32


def solution(mesh):
    placed = (
        P("vid", "seg", "tp"),
        P("vid", "tp"),
        P("vid", "tp"),
        P(None, "tp"),
        P("vid", None, "tp"),
        P("vid", "seg", "tp"),
    )
    sizes = tuple(mesh.shape[axis] for axis in ("seg", "vid", "tp"))
    body = functools.partial(fused_shards, sizes) if relay_fits(*sizes) else shards
    return jax.shard_map(
        body,
        mesh=mesh,
        in_specs=placed,
        out_specs=(P("vid", "seg", "tp"), P("vid", "seg", "tp")),
        check_vma=False,
    )
```

```python
import functools

import jax
import jax.numpy as jnp
from jax import lax
from jax.experimental import pallas as pl
from jax.experimental.pallas import tpu as pltpu
from jax.sharding import PartitionSpec as P

HEAD = 128


def from_behind(block, axis, distance):
    devices = range(lax.axis_size(axis))
    route = [(i - distance, i) for i in devices if i - distance in devices]
    return lax.ppermute(block, axis, route)


def trailing_softmax(scores):
    top = jnp.max(scores, axis=-1, keepdims=True)
    expo = jnp.exp(scores - top)
    return expo / jnp.sum(expo, axis=-1, keepdims=True)


def add_rows(left, piece):
    return jnp.dot(left, piece, preferred_element_type=jnp.float32)


def shards(tokens, key_weight, query_weight, latent_queries, init_memory, forget):
    local = tokens[0]
    width = local.shape[1]
    heads = width // HEAD
    latents = latent_queries.shape[0]
    whole = lax.all_gather(local, "tp", axis=1, tiled=True)

    def add_one(piece):
        return add_rows(whole, piece)

    keys_full = add_one(lax.all_gather(key_weight, "vid", axis=0, tiled=True))
    queries_full = add_one(lax.all_gather(query_weight, "vid", axis=0, tiled=True))
    scale = 1.0 / jnp.sqrt(jnp.float32(HEAD))
    keys = keys_full.astype(jnp.bfloat16).reshape(-1, heads, HEAD)
    queries = queries_full.astype(jnp.bfloat16).reshape(-1, heads, HEAD)
    values = local.reshape(-1, heads, HEAD)
    latent = latent_queries.reshape(latents, heads, HEAD)
    scores = jnp.einsum("mhe,the->hmt", latent, keys, preferred_element_type=jnp.float32) * scale
    weight_params = trailing_softmax(scores).astype(jnp.bfloat16)
    update = jnp.einsum(
        "hmt,the->mhe", weight_params, values, preferred_element_type=jnp.float32
    ).reshape(latents, width)
    retain = forget[0]
    initial_memory = init_memory[0]
    first = lax.axis_index("seg") == 0

    def turn(step, memory_now):
        received = from_behind(retain * memory_now + update, "seg", 1)
        return jnp.where(first, initial_memory, received)

    memory_in = lax.fori_loop(0, lax.axis_size("seg") - 1, turn, initial_memory)
    memory_out = retain * memory_in + update
    grouped = memory_in.reshape(latents, heads, HEAD)
    normed = grouped * lax.rsqrt(jnp.mean(grouped * grouped, axis=-1, keepdims=True) + 1e-06)
    read_scores = (
        jnp.einsum(
            "the,mhe->htm", queries, normed.astype(jnp.bfloat16), preferred_element_type=jnp.float32
        )
        * scale
    )
    read_weights = trailing_softmax(read_scores).astype(jnp.bfloat16)
    read = jnp.einsum(
        "htm,mhe->the",
        read_weights,
        grouped.astype(jnp.bfloat16),
        preferred_element_type=jnp.float32,
    )
    mixed = (local.astype(jnp.float32) + read.reshape(-1, width)).astype(jnp.bfloat16)
    return (mixed[None], memory_out[None])


CORES = 2
TILE = 2 * HEAD
AHEAD = 3
SKEW = 1
HOLD = 0
BEHIND = 4
LATE = 4
DIRECT = 2
EARLY = 1
STEP = 0
LAGS = (0, 1, 6, 7)
GROUP = 4


def softmax_rows(scores):
    top = jnp.max(scores, axis=-1, keepdims=True)
    expo = jnp.exp(scores - top)
    return (expo * (1.0 / jnp.sum(expo, axis=-1, keepdims=True))).astype(jnp.bfloat16)


def fused_kernel(
    segs, vids, tps,
    tokens, key_w, query_w, latent_in, init_memory, forget_in,
    mixed, memory_out,
    weights, tok, queries, memory_in, update, partial, raised, flipped, latent, forget,
    load_sem, tok_send, tok_recv, z_send, z_recv, y_send, y_recv, d_send, d_recv, m_send, m_recv,
):
    s, z, t = lax.axis_index("seg"), lax.axis_index("vid"), lax.axis_index("tp")
    y, core = s // CORES, s % CORES
    partner = y * CORES + (1 - core)
    across = (1 - y) * CORES + core
    count, width = tokens.shape
    tiles = width // TILE
    blocks = vids // tps
    depth = blocks * weights.shape[2] * weights.shape[3]
    chunks = range(2 * tiles)
    sides = (1, -1)

    def remote(src, dst, send, recv, device):
        return pltpu.make_async_remote_copy(
            src_ref=src, dst_ref=dst, send_sem=send, recv_sem=recv,
            device_id=device, device_id_type=pl.DeviceIdType.MESH,
        )

    def tile_cols(k):
        return pl.ds(k % tiles * TILE, TILE)

    def lanes(k):
        return (s, across) if k >= len(chunks) - DIRECT else (s,)

    def z_copy(k, source, side, lane):
        block = weights.at[k, source, lanes(k)[lane]]
        return remote(
            block, block, z_send.at[k, source, (1 - side) // 2, lane], z_recv.at[k, source, lane], {"vid": z + side}
        )

    def through(source, side):
        return (vids - 1 - source if side == 1 else source) > 1

    def y_copy(k, source, owner):
        block = weights.at[k, source, owner]
        return remote(block, block, y_send.at[k, source], y_recv.at[k, source], {"seg": across})

    def d_copy(k, source, owner, kind):
        block = weights.at[k, source, owner]
        return remote(block, block, d_send.at[k, source, kind], d_recv.at[k, source, kind], {"seg": partner})

    def m_copy(c, device):
        cols = tile_cols(c)
        return remote(memory_out.at[:, cols], memory_in.at[:, cols], m_send.at[c], m_recv.at[c], {"seg": device})

    def inside(index, size):
        return (index >= 0) & (index < size)

    def flag(condition):
        return jnp.where(condition, 1, 0).astype(jnp.int32)

    loads = [
        pltpu.make_async_copy(
            (key_w, query_w)[k // tiles].at[:, :, tile_cols(k)], weights.at[k, z], load_sem.at[k]
        )
        for k in chunks
    ]
    tok_load = pltpu.make_async_copy(tokens, tok.at[t], load_sem.at[len(loads)])
    first_memory = pltpu.make_async_copy(init_memory, memory_in, load_sem.at[len(loads) + 1])
    latent_load = pltpu.make_async_copy(latent_in, latent, load_sem.at[len(loads) + 2])
    forget_load = pltpu.make_async_copy(forget_in, forget, load_sem.at[len(loads) + 3])
    for load in loads[:1] + [tok_load] + loads[1:] + [latent_load, forget_load]:
        load.start()

    @pl.when(s == 0)
    def _():
        first_memory.start()

    barrier = pltpu.get_barrier_semaphore()
    greeted = [
        (z + 1 < vids, {"vid": z + 1}),
        (z > 0, {"vid": z - 1}),
        (s >= 0, {"seg": across}),
        ((core == 1) & (y == 0), {"seg": s + 1}),
        ((core == 0) & (y == 1), {"seg": s - 1}),
        (s >= 0, {"seg": partner}),
        (s >= 0, {"tp": 1 - t}),
    ]
    waited = 0
    for condition, device in greeted:
        waited = waited + flag(condition)

        @pl.when(condition)
        def _(device=device):
            pl.semaphore_signal(barrier, inc=1, device_id=device, device_id_type=pl.DeviceIdType.MESH)

    pl.semaphore_wait(barrier, waited)

    def own_sends(k):
        for side in sides:
            @pl.when(inside(z + side, vids))
            def _(side=side):
                z_copy(k, z, side, 0).start()

            if len(lanes(k)) > 1:
                @pl.when(inside(z + side, vids) & through(z, side))
                def _(side=side):
                    z_copy(k, z, side, 1).start()

    tok_copy = remote(tok.at[t], tok.at[t], tok_send, tok_recv, {"tp": 1 - t})
    for k in chunks[:AHEAD]:
        loads[k].wait()
        own_sends(k)
        if k == 0:
            tok_load.wait()
            tok_copy.start()
    for k in chunks[AHEAD:]:
        loads[k].wait()
    latent_load.wait()
    forget_load.wait()

    @pl.when(s == 0)
    def _():
        first_memory.wait()

    def each_source(distance, action):
        for side in sides:
            source = z - side * distance

            @pl.when(inside(source, vids))
            def _(source=source, side=side):
                action(source, side)

    def arrive_z(k, distance):
        def action(source, side):
            def take(lane):
                z_copy(k, source, side, lane).wait_recv()

                @pl.when(inside(z + side, vids))
                def _():
                    z_copy(k, source, side, lane).start()

                d_copy(k, source, (s, across)[lane], lane).start()

            take(0)
            if len(lanes(k)) == 1:
                y_copy(k, source, s).start()
            elif distance > 1:
                take(1)
            else:
                @pl.when(through(source, side))
                def _():
                    take(1)

                @pl.when(jnp.logical_not(through(source, side)))
                def _():
                    y_copy(k, source, s).start()

        each_source(distance, action)
        if distance == 1 and k + AHEAD < len(chunks):
            own_sends(k + AHEAD)

    def arrive_y(k, distance):
        def action(source, side):
            def take():
                y_copy(k, source, across).wait_recv()
                d_copy(k, source, across, 1).start()

            if len(lanes(k)) == 1:
                take()
            else:
                pl.when(jnp.logical_not(through(source, side)))(take)

        each_source(distance, action)

    def arrive_d(k):
        for distance in range(1, vids):
            def action(source, side):
                d_copy(k, source, partner, 0).wait_recv()
                d_copy(k, source, (1 - y) * CORES + 1 - core, 1).wait_recv()

            each_source(distance, action)

    def half_product(k, half):
        right = weights[k, pl.ds(half * blocks, blocks)].reshape(depth, TILE)
        return jnp.dot(tok[half], right, preferred_element_type=jnp.float32)

    scale = 1.0 / jnp.sqrt(jnp.float32(HEAD))

    def flip(k):
        flipped[tile_cols(k)] = tok[t, :, tile_cols(k)].T

    def key_near(k):
        arrive_d(k)
        partial[k] = half_product(k, t)

    def key_far(k):
        keys = (partial[k] + half_product(k, 1 - t)).astype(jnp.bfloat16)
        for h in range(TILE // HEAD):
            cols = pl.ds(k * TILE + h * HEAD, HEAD)
            raised[:, cols] = lax.dot_general(
                keys[:, h * HEAD:(h + 1) * HEAD], latent[:, cols], (((1,), (1,)), ((), ())),
                preferred_element_type=jnp.float32,
            ) * scale

    def blend(group):
        at = group[0] * TILE
        span = len(group) * TILE
        scores = raised[:, at:at + span]
        expo = jnp.exp(scores - jnp.max(scores, axis=0, keepdims=True))
        held = (expo * (1.0 / jnp.sum(expo, axis=0, keepdims=True))).astype(jnp.bfloat16)
        for h in range(span // HEAD):
            cols = pl.ds(at + h * HEAD, HEAD)
            update[:, cols] = jnp.dot(
                flipped[cols], held[:, h * HEAD:(h + 1) * HEAD], preferred_element_type=jnp.float32
            ).T

    def carry(c, seg):
        cols = tile_cols(c)

        @pl.when(s == seg)
        def _():
            if seg > 0:
                m_copy(c, s - 1).wait_recv()
            memory_out[:, cols] = forget[:, cols] * memory_in[:, cols] + update[:, cols]
            if seg + 1 < segs:
                m_copy(c, s + 1).start()

    def query(k):
        arrive_d(k)
        queries[:, tile_cols(k)] = (half_product(k, t) + half_product(k, 1 - t)).astype(jnp.bfloat16)

    def readout(k):
        for h in range(TILE // HEAD):
            cols = pl.ds(k % tiles * TILE + h * HEAD, HEAD)
            held = memory_in[:, cols]
            normed = held * lax.rsqrt(jnp.mean(held * held, axis=-1, keepdims=True) + 1e-06)
            scores = lax.dot_general(
                queries[:, cols], normed.astype(jnp.bfloat16), (((1,), (1,)), ((), ())),
                preferred_element_type=jnp.float32,
            )
            read = jnp.dot(softmax_rows(scores * scale), held.astype(jnp.bfloat16), preferred_element_type=jnp.float32)
            mixed[:, cols] = (tok[t, :, cols].astype(jnp.float32) + read).astype(jnp.bfloat16)

    def far_tokens():
        remote(tok.at[1 - t], tok.at[1 - t], tok_send, tok_recv, {"tp": 1 - t}).wait_recv()

    gaps = vids - 1
    slots = [(k, distance) for k in chunks for distance in range(1, vids)]
    slots.sort(key=lambda slot: (slot[0] + SKEW * (slot[1] - 1) + HOLD * (slot[0] >= tiles), slot[1]))
    relays = [
        (at + (BEHIND if slot[0] < tiles else LATE), slot) for at, slot in enumerate(slots)
        if len(lanes(slot[0])) == 1 or slot[1] == 1
    ]
    done = {k: slots.index((k, gaps)) + 1 for k in chunks}
    for at, (k, _) in relays:
        done[k] = max(done[k], at + 1)
    plan = []

    def place(at, task, *args):
        plan.append((at, task, args))

    start = done[tiles - 1] - EARLY
    for k in range(tiles):
        place(k + 1, flip, k)
        place(done[k], key_near, k)
    place(start, far_tokens)
    for k in range(tiles):
        place(max(start, done[k]) + STEP * k, key_far, k)
    mixed_at = max(start, done[tiles - 1]) + STEP * (tiles - 1)
    for at in range(0, tiles, GROUP):
        place(mixed_at, blend, range(at, min(at + GROUP, tiles)))
    for k in range(tiles):
        for seg, lag in enumerate(LAGS):
            place(mixed_at + lag, carry, k, seg)
    for k in range(tiles, 2 * tiles):
        place(done[k], query, k)
        place(max(done[k // 2 * 2 + 1], mixed_at + LAGS[-1]), readout, k)
    for at, slot in enumerate(slots):
        place(at - 0.2, arrive_z, *slot)
    for at, slot in relays:
        place(at - 0.1, arrive_y, *slot)
    for at, task, args in sorted(plan, key=lambda entry: entry[0]):
        task(*args)

    tok_copy.wait_send()
    for k in chunks:
        for side in sides:
            @pl.when(inside(z + side, vids))
            def _(k=k, side=side):
                z_copy(k, z, side, 0).wait_send()

            if len(lanes(k)) > 1:
                @pl.when(inside(z + side, vids) & through(z, side))
                def _(k=k, side=side):
                    z_copy(k, z, side, 1).wait_send()

        for distance in range(1, vids):
            def sent(source, side, k=k):
                @pl.when(inside(z + side, vids))
                def _():
                    for lane in range(len(lanes(k))):
                        z_copy(k, source, side, lane).wait_send()

                if len(lanes(k)) == 1:
                    y_copy(k, source, s).wait_send()
                elif distance == 1:
                    @pl.when(jnp.logical_not(through(source, side)))
                    def _():
                        y_copy(k, source, s).wait_send()

                d_copy(k, source, s, 0).wait_send()
                d_copy(k, source, across, 1).wait_send()

            each_source(distance, sent)

    @pl.when(s + 1 < segs)
    def _():
        for c in range(tiles):
            m_copy(c, s + 1).wait_send()


def fused_shards(sizes, tokens, key_weight, query_weight, latent_queries, init_memory, forget):
    segs, vids, tps = sizes
    local = tokens[0]
    count, width = local.shape
    latents = latent_queries.shape[0]
    rows = key_weight.shape[0]
    tiles = width // TILE
    parts = (segs, rows // segs, width)
    hbm = pl.BlockSpec(memory_space=pltpu.HBM)
    vmem = pl.BlockSpec(memory_space=pltpu.VMEM)
    dma = pltpu.SemaphoreType.DMA
    mixed, memory = pl.pallas_call(
        functools.partial(fused_kernel, segs, vids, tps),
        out_shape=(
            jax.ShapeDtypeStruct((count, width), jnp.bfloat16),
            jax.ShapeDtypeStruct((latents, width), jnp.float32),
        ),
        in_specs=[hbm] * 6,
        out_specs=(vmem, vmem),
        scratch_shapes=[
            pltpu.VMEM((2 * tiles, vids, segs, rows // segs, TILE), jnp.bfloat16),
            pltpu.VMEM((tps, count, width), jnp.bfloat16),
            pltpu.VMEM((count, width), jnp.bfloat16),
            pltpu.VMEM((latents, width), jnp.float32),
            pltpu.VMEM((latents, width), jnp.float32),
            pltpu.VMEM((tiles, count, TILE), jnp.float32),
            pltpu.VMEM((count, width), jnp.float32),
            pltpu.VMEM((width, count), jnp.bfloat16),
            pltpu.VMEM((latents, width), jnp.bfloat16),
            pltpu.VMEM((1, width), jnp.float32),
            dma((2 * tiles + 4,)),
            dma,
            dma,
            dma((2 * tiles, vids, 2, 2)),
            dma((2 * tiles, vids, 2)),
            dma((2 * tiles, vids)),
            dma((2 * tiles, vids)),
            dma((2 * tiles, vids, 2)),
            dma((2 * tiles, vids, 2)),
            dma((tiles,)),
            dma((tiles,)),
        ],
        compiler_params=pltpu.CompilerParams(
            collective_id=0, has_side_effects=True, vmem_limit_bytes=GRANT
        ),
    )(
        *(
            pltpu.with_memory_space_constraint(array, pltpu.HBM)
            for array in (
                local, key_weight.reshape(parts), query_weight.reshape(parts), latent_queries, init_memory[0], forget[0]
            )
        )
    )
    return (mixed[None], memory[None])


GRANT = 28 * 1024 * 1024


def relay_fits(segs, vids, tps):
    return tps == 2 and segs == 2 * CORES and vids > 2 and vids % tps == 0 and segs * vids <= 32


def solution(mesh):
    placed = (
        P("vid", "seg", "tp"),
        P("vid", "tp"),
        P("vid", "tp"),
        P(None, "tp"),
        P("vid", None, "tp"),
        P("vid", "seg", "tp"),
    )
    sizes = tuple(mesh.shape[axis] for axis in ("seg", "vid", "tp"))
    body = functools.partial(fused_shards, sizes) if relay_fits(*sizes) else shards
    return jax.shard_map(
        body,
        mesh=mesh,
        in_specs=placed,
        out_specs=(P("vid", "seg", "tp"), P("vid", "seg", "tp")),
        check_vma=False,
    )
```
